256 devices in a mesh: hist: 32 (over x, z_hi, y), row: 4 (over z_lo), cur: 2 (over core).
Axes of the slice: x: 4, y: 4, z: 8 (z_hi: 2, z_lo: 4; z = z_hi * 4 + z_lo), core: 2. Of those that a mesh axis runs over, the one named last changes fastest.
Arguments:
- incident: bfloat16 [4, 256, 256, 64], P(None, ('hist', 'row', 'cur')), may hold values from -6 to 6
- past: bfloat16 [256, 8, 256, 64], P(('hist', 'row', 'cur')), may hold values from -6 to 6
- hist_tiles: bfloat16 [256, 64, 256, 256], P(('hist', 'row', 'cur')), may hold values from -0.046875 to 0.046875
- tile_rows: int32 [256, 64], P(('hist', 'row', 'cur')), may hold values from 0 to 31
- tile_cols: int32 [256, 64], P(('hist', 'row', 'cur')), may hold values from 0 to 7
- tile_lags: int32 [256, 64], P(('hist', 'row', 'cur')), may hold values from 4 to 8
- tile_scales: float32 [256, 64], P(('hist', 'row', 'cur')), may hold values from 0.5 to 2
- near_tiles: bfloat16 [256, 3, 5, 256, 256], P(('hist', 'row', 'cur')), may hold values from -0.09375 to 0.09375
- inverses: bfloat16 [256, 256, 256], P(('hist', 'row', 'cur')), may hold values from -0.21875 to 0.21875
Outputs:
- densities: bfloat16 [4, 256, 256, 64], P(None, ('hist', 'row', 'cur'))
The draws below stay inside these ranges and needn't reach their ends.
All inputs are finite; a program needn't handle non-finite values.
Results may differ from the reference program's by a relative error of at most 0.02.
Values may be sent and summed in bfloat16 or wider, within the bound.
A program may use at most 128 MiB of HBM per device.

```python
import math
import jax
import jax.numpy as jnp
from jax import lax

BLOCK = 256
ILLUM = 64
STEPS = 4
LAGS = 8
TILES_DEV = 64
PATCHES = 256
GROUPS = 32
LOCAL = 8
N_ROW = 4
N_CUR = 2


def plant(entries, rng, least, high):
    longest = entries.shape.index(max(entries.shape))
    spots = []
    for shift in (0, 1):
        where = [jax.random.randint(jax.random.fold_in(rng, axis), (), 0, length) for axis, length in enumerate(entries.shape)]
        where[longest] = (where[longest] + shift) % entries.shape[longest]
        spots.append(tuple(where))
    return entries.at[spots[0]].set(least).at[spots[1]].set(high)


def shard_levels(rng, dims, shards, smallest, top_value):
    def one(axis_at, parts):
        heights = jax.random.uniform(jax.random.fold_in(jax.random.fold_in(rng, 6), axis_at), (parts,), jnp.float32, smallest / len(shards), top_value / len(shards))
        return jnp.repeat(jnp.exp(heights), dims[axis_at] // parts).reshape((-1,) + (1,) * (len(dims) - axis_at - 1))

    loudness = one(*shards[0])
    for cut in shards[1:]:
        loudness = loudness * one(*cut)
    return loudness


def scatter_about(key, dims, scale, reach, shards=(), held_as=jnp.bfloat16):
    drawn = jax.random.normal(key, dims, jnp.float32) * scale
    if len(shards) > 0:
        drawn = shard_levels(key, dims, shards, -0.22, 0.18) * drawn
    return jnp.clip(drawn, min=-reach, max=reach).astype(held_as)


def setup_inputs(seed: int = 0) -> dict:
    keys = jax.random.split(jax.random.key(seed), 10)
    incident = scatter_about(keys[0], (STEPS, PATCHES, BLOCK, ILLUM), 1.0, 6.0, ((1, 256),))
    past = scatter_about(keys[1], (PATCHES, LAGS, BLOCK, ILLUM), 1.0, 6.0, ((0, 256),))
    hist_tiles = scatter_about(keys[2], (PATCHES, TILES_DEV, BLOCK, BLOCK), (TILES_DEV * BLOCK) ** -0.5, 0.046875, ((0, 256),))
    tile_rows = plant(jax.random.randint(keys[3], (PATCHES, TILES_DEV), 0, GROUPS), jax.random.fold_in(keys[3], 1), 0, GROUPS - 1).astype(jnp.int32)
    tile_cols = plant(jax.random.randint(keys[4], (PATCHES, TILES_DEV), 0, LOCAL), jax.random.fold_in(keys[4], 1), 0, LOCAL - 1).astype(jnp.int32)
    tile_lags = plant(jax.random.randint(keys[5], (PATCHES, TILES_DEV), 4, 9), jax.random.fold_in(keys[5], 1), 4, 8).astype(jnp.int32)
    tile_scales = jnp.clip(jnp.exp(math.log(2.0) - 1.3862944 * jax.random.uniform(keys[6], (PATCHES, TILES_DEV), jnp.float32) ** shard_levels(keys[6], (PATCHES, TILES_DEV), ((0, 256),), -0.2, 0.2)), 0.5, 2.0)
    near_tiles = scatter_about(keys[7], (PATCHES, 3, 5, BLOCK, BLOCK), (15 * BLOCK) ** -0.5, 0.09375, ((0, 256),))
    inverses = scatter_about(keys[8], (PATCHES, BLOCK, BLOCK), (3 * BLOCK) ** -0.5, 0.21875, ((0, 256),))
    return dict(incident=incident, past=past, hist_tiles=hist_tiles, tile_rows=tile_rows, tile_cols=tile_cols, tile_lags=tile_lags, tile_scales=tile_scales, near_tiles=near_tiles, inverses=inverses)


def reference(incident, past, hist_tiles, tile_rows, tile_cols, tile_lags, tile_scales, near_tiles, inverses):
    local_count = N_ROW * N_CUR
    step_ids = jnp.arange(STEPS, dtype=jnp.int32)

    def per_holder(total, holder):
        group = holder // local_count
        slot = holder % local_count
        source = group * local_count + tile_cols[holder]
        when = step_ids[:, None] - tile_lags[holder][None, :] + LAGS
        picked = past[source[None, :], when]
        terms = jnp.einsum('kij,skjr->skir', hist_tiles[holder].astype(jnp.float32), picked.astype(jnp.float32))
        terms = terms * tile_scales[holder][None, :, None, None]
        target = tile_rows[holder] * local_count + slot
        return total.at[:, target].add(terms), None

    start = jnp.zeros((STEPS, PATCHES, BLOCK, ILLUM), jnp.float32)
    history, _ = lax.scan(per_holder, start, jnp.arange(PATCHES, dtype=jnp.int32))

    made = []
    for step in range(STEPS):
        near = jnp.zeros((PATCHES, BLOCK, ILLUM), jnp.float32)
        for lag in range(1, 4):
            when = step - lag
            earlier = past[:, when + LAGS] if when < 0 else made[when]
            padded = jnp.pad(earlier, ((2, 2), (0, 0), (0, 0)))
            for offset in range(-2, 3):
                beside = padded[2 + offset:2 + offset + PATCHES]
                near = near + jnp.einsum('pij,pjr->pir', near_tiles[:, lag - 1, offset + 2].astype(jnp.float32), beside.astype(jnp.float32))
        rhs = (incident[step].astype(jnp.float32) - history[step] - near).astype(jnp.bfloat16)
        fresh = jnp.einsum('pij,pjr->pir', inverses.astype(jnp.float32), rhs.astype(jnp.float32)).astype(jnp.bfloat16)
        made.append(fresh)
    return jnp.stack(made)
```

```python
import functools

import jax
import jax.numpy as jnp
from jax import lax
from jax.experimental import pallas as pl
from jax.experimental.pallas import tpu as pltpu
from jax.sharding import Mesh
from jax.sharding import PartitionSpec as P

AXES = ("hist_0", "hist_1", "hist_2", "row", "cur")
MESH = pl.DeviceIdType.MESH
F32 = jnp.float32
BF16 = jnp.bfloat16
STEPS = 4
HALF = 32
ILLUM = 64
BLOCK = 256
TILES = 64
GROUPS = 32
PATCHES = 256
TILE_PARTS = 8


def times_transposed(x, w):
    return lax.dot_general(x, w, (((1,), (1,)), ((), ())), preferred_element_type=F32)


def kernel(
    info_ref, scale_ref, end_ref,
    past_ref, tiles_ref, near_ref, inverse_ref, incident_ref,
    out_ref,
    tiles, near, inverse, incident, gp, acc, slots, pa, pb,
    rel1, dir1, s1, rel2, dir2, ts, hist, zr, window, fresh, pre,
    local_sem, g_send, g_recv, d_send, d_recv,
    r_send, r_recv, z_send, z_recv, w_send, w_recv, n_send, n_recv,
):
    x = lax.axis_index("hist_0")
    zh = lax.axis_index("hist_1")
    y = lax.axis_index("hist_2")
    row = lax.axis_index("row")
    cur = lax.axis_index("cur")
    me = (((x * 2 + zh) * 4 + y) * 4 + row) * 2 + cur
    own = row * 2 + cur

    def patch_device(offset):
        q = lax.rem(me + offset + PATCHES, PATCHES)
        return {
            "hist_0": q // 64,
            "hist_1": lax.rem(q // 32, 2),
            "hist_2": lax.rem(q // 8, 4),
            "row": lax.rem(q // 2, 4),
            "cur": lax.rem(q, 2),
        }

    barrier = pltpu.get_barrier_semaphore()

    first = pltpu.make_async_copy(past_ref, gp.at[own], local_sem.at[0])
    first.start()
    loads = []
    part = TILES // TILE_PARTS
    for k in range(TILE_PARTS):
        loads.append(
            pltpu.make_async_copy(
                tiles_ref.at[pl.ds(k * part, part)],
                tiles.at[pl.ds(k * part, part)],
                local_sem.at[4 + k],
            )
        )
    near_load = pltpu.make_async_copy(near_ref, near, local_sem.at[1])
    inverse_load = pltpu.make_async_copy(inverse_ref, inverse, local_sem.at[2])
    incident_load = pltpu.make_async_copy(incident_ref, incident, local_sem.at[3])

    partners = [
        {"hist_0": lax.rem(x + 1, 4)},
        {"hist_0": lax.rem(x + 3, 4)},
        {"hist_2": lax.rem(y + 1, 4)},
        {"hist_2": lax.rem(y + 3, 4)},
        {"hist_1": 1 - zh},
        {"row": lax.rem(row + 1, 4)},
        {"row": lax.rem(row + 2, 4)},
        {"row": lax.rem(row + 3, 4)},
        {"cur": 1 - cur},
        patch_device(1),
        patch_device(2),
        patch_device(-1),
        patch_device(-2),
    ]
    for device in partners:
        pl.semaphore_signal(barrier, inc=1, device_id=device, device_id_type=MESH)
    pl.semaphore_wait(barrier, len(partners))
    first.wait()

    def remote(src, dst, send, recv, device):
        return pltpu.make_async_remote_copy(
            src_ref=src, dst_ref=dst, send_sem=send, recv_sem=recv,
            device_id=device, device_id_type=MESH,
        )

    inner = lax.rem((row + 1) // 2, 2)
    opposite = lax.rem(row + 2, 4)
    middle = 1 + lax.rem(row, 2)
    outer = 3 * (row // 2)
    blocks = [opposite, 1 + lax.rem(row, 2), 3 - 3 * lax.rem(row, 2)]
    to_opposite = remote(gp.at[own], gp.at[own], g_send.at[0], g_recv.at[0], {"row": opposite})
    to_middle = remote(
        gp.at[own], gp.at[own], g_send.at[1], g_recv.at[2 - inner], {"row": middle}
    )
    to_outer = remote(gp.at[own], gp.at[own], g_send.at[2], g_recv.at[1], {"row": outer})
    far = opposite * 2 + cur
    relayed = remote(gp.at[far], gp.at[far], g_send.at[3], g_recv.at[2], {"row": outer})
    to_opposite.start()
    to_middle.start()

    @pl.when(inner == 1)
    def _():
        to_outer.start()

    across = []
    for k, block in enumerate([row] + blocks):
        spot = gp.at[block * 2 + cur]
        across.append(remote(spot, spot, d_send.at[k], d_recv.at[k], {"cur": 1 - cur}))
    across[0].start()
    for load in loads:
        load.start()
    near_load.start()
    inverse_load.start()
    incident_load.start()

    def arrived(k):
        spot = gp.at[blocks[k] * 2 + cur]
        remote(spot, spot, g_send.at[k], g_recv.at[k], {"row": opposite}).wait_recv()

    arrived(0)

    @pl.when(inner == 1)
    def _():
        relayed.start()

    across[1].start()

    offsets = (-2, -1, 1, 2)
    window_sends = []
    for k, o in enumerate(offsets):
        window_sends.append(
            remote(
                gp.at[own, pl.ds(5, 3)], window.at[o + 2, pl.ds(0, 3)],
                w_send.at[k], w_recv.at[k], patch_device(-o),
            )
        )
    arrived(1)
    across[2].start()
    arrived(2)
    across[3].start()
    for send in window_sends:
        send.start()
    window[2, pl.ds(0, 3)] = gp[own, pl.ds(5, 3)]
    for load in loads:
        load.wait()
    for copy in across:
        copy.wait_recv()

    acc[...] = jnp.zeros_like(acc)

    def one_tile(k, carry):
        tile = info_ref[0, k]
        col = info_ref[1, k]
        begin = info_ref[2, k]
        held = gp[col, pl.ds(begin, STEPS)].reshape(STEPS * ILLUM, BLOCK)
        term = times_transposed(held, tiles[tile]) * scale_ref[0, k]
        total = acc[...] * scale_ref[1, k] + term
        acc[...] = total
        slots[k] = total.astype(BF16)
        return carry

    lax.fori_loop(0, TILES, one_tile, 0, unroll=2)

    def spread(t):
        def one_group(g, carry):
            end = end_ref[0, g]
            there = end_ref[1, g]
            value = slots[end, pl.ds(t * ILLUM, ILLUM)]
            value = jnp.where(there > 0, value, jnp.zeros_like(value))
            gx = g // 8
            gz = lax.rem(g // 4, 2)
            gy = lax.rem(g, 4)
            pa[t, gx, gz, gy] = value[:HALF]
            pb[t, gy, gz, gx] = value[HALF:]
            return carry

        lax.fori_loop(0, GROUPS, one_group, 0, unroll=4)

    rings = (("hist_0", x), ("hist_2", y))
    sends = []

    def ring_copy(t, stage, h, n, src, dst, device):
        index = ((t * 2 + stage) * 2 + h) * 6 + n
        copy = remote(src, dst, r_send.at[index], r_recv.at[index], device)
        sends.append(copy)
        return copy

    def ring(t, stage, h):
        axis, i = rings[(h + stage) % 2]
        right, left, over = lax.rem(i + 1, 4), lax.rem(i + 3, 4), lax.rem(i + 2, 4)
        if stage == 0:
            source = (pa, pb)[h]
            at = lambda j, z: source.at[t, j, z]
            rel, dirs = rel1, dir1
        else:
            at = lambda j, z: s1.at[h, t, z, j]
            rel, dirs = rel2, dir2
        to_right, to_left = {axis: right}, {axis: left}
        copies = (
            ring_copy(t, stage, h, 0, at(over, 0), rel.at[h, 0, t], to_right),
            ring_copy(t, stage, h, 1, at(over, 1), rel.at[h, 1, t], to_left),
            ring_copy(t, stage, h, 2, at(right, 1), dirs.at[h, 0, t, 1], to_right),
            ring_copy(t, stage, h, 3, at(left, 0), dirs.at[h, 1, t, 0], to_left),
            ring_copy(t, stage, h, 4, at(right, 0), dirs.at[h, 0, t, 0], to_right),
            ring_copy(t, stage, h, 5, at(left, 1), dirs.at[h, 1, t, 1], to_left),
        )
        return copies, at, rel, dirs, right, left, i

    state = {}

    def start(t, stage):
        for h in (0, 1):
            state[t, stage, h] = ring(t, stage, h)
        for n in (0, 1, 2, 3):
            for h in (0, 1):
                state[t, stage, h][0][n].start()

    def relay(t, stage):
        for n, z in ((0, 0), (1, 1)):
            for h in (0, 1):
                copies, at, rel, dirs, right, left, i = state[t, stage, h]
                copies[n].wait_recv()
                spot = at((right, left)[n], z)
                spot[...] = (spot[...].astype(F32) + rel[h, n, t].astype(F32)).astype(BF16)
                copies[4 + n].start()

    def finish_first(t):
        for h in (0, 1):
            copies, at, rel, dirs, right, left, i = state[t, 0, h]
            for n in (2, 3, 4, 5):
                copies[n].wait_recv()
            for z in (0, 1):
                total = at(i, z)[...].astype(F32) + dirs[h, 0, t, z].astype(F32)
                s1[h, t, z] = (total + dirs[h, 1, t, z].astype(F32)).astype(BF16)

    pairs = {}

    def finish_second(t):
        for h in (0, 1):
            copies, at, rel, dirs, right, left, i = state[t, 1, h]
            for n in (2, 3, 4, 5):
                copies[n].wait_recv()

        def total(h, z):
            copies, at, rel, dirs, right, left, i = state[t, 1, h]
            return at(i, z)[...].astype(F32) + dirs[h, 0, t, z].astype(F32) + dirs[h, 1, t, z].astype(F32)

        for h in (0, 1):
            ts[t, pl.ds(h * HALF, HALF)] = total(h, 1 - zh).astype(BF16)
        pairs[t] = remote(ts.at[t], zr.at[t], z_send.at[t], z_recv.at[t], {"hist_1": 1 - zh})
        sends.append(pairs[t])
        pairs[t].start()
        for h in (0, 1):
            hist[t, pl.ds(h * HALF, HALF)] = total(h, zh)

    valid = {o: jnp.logical_and(me + o >= 0, me + o < PATCHES) for o in offsets}

    def beside(o, s):
        value = window[o + 2, s + 3]
        if o == 0:
            return value
        return jnp.where(valid[o], value, jnp.zeros_like(value))

    def near_sum(lag, s, chosen):
        total = None
        for o in chosen:
            term = times_transposed(beside(o, s), near[(lag - 1) * 5 + o + 2])
            total = term if total is None else total + term
        return total

    everyone = (-2, -1, 0, 1, 2)
    rounds = {}

    def start_pre():
        near_load.wait()
        inverse_load.wait()
        incident_load.wait()
        for send in window_sends:
            send.wait_recv()
        for t in range(STEPS):
            total = incident[t].astype(F32)
            for lag in range(1, 4):
                if t - lag < 0:
                    total = total - near_sum(lag, t - lag, everyone)
            pre[t] = total

    def near_step(t):
        total = pre[t]
        if t > 0:
            for copy in rounds[t - 1]:
                copy.wait_recv()
            total = total - near_sum(1, t - 1, offsets)
        if t == 0 or True:
            pairs[t].wait_recv()
        rhs = (total - hist[t] - zr[t].astype(F32)).astype(BF16)
        made = times_transposed(rhs, inverse[...]).astype(BF16)
        out_ref[t] = made
        if t + 1 < STEPS:
            fresh[t] = made
            rounds[t] = []
            for k, o in enumerate(offsets):
                copy = remote(
                    fresh.at[t], window.at[o + 2, t + 3],
                    n_send.at[t * 4 + k], n_recv.at[t * 4 + k], patch_device(-o),
                )
                copy.start()
                rounds[t].append(copy)
                sends.append(copy)
            window[2, t + 3] = made
            pre[t + 1] = pre[t + 1] - near_sum(1, t, (0,))
        if t > 0:
            for lag in (2, 3):
                if t - 1 + lag < STEPS:
                    pre[t - 1 + lag] = pre[t - 1 + lag] - near_sum(lag, t - 1, everyone)

    spread(0)
    start(0, 0)
    spread(1)
    start(1, 0)
    spread(2)
    spread(3)
    relay(0, 0)
    start(2, 0)
    relay(1, 0)
    finish_first(0)
    start(0, 1)
    start(3, 0)
    start_pre()
    relay(2, 0)
    relay(0, 1)
    finish_first(1)
    start(1, 1)
    finish_second(0)
    relay(3, 0)
    relay(1, 1)
    finish_first(2)
    start(2, 1)
    near_step(0)
    finish_second(1)
    relay(2, 1)
    finish_first(3)
    start(3, 1)
    near_step(1)
    finish_second(2)
    relay(3, 1)
    near_step(2)
    finish_second(3)
    near_step(3)

    for copy in sends:
        copy.wait_send()
    for copy in window_sends:
        copy.wait_send()
    for copy in across:
        copy.wait_send()
    to_opposite.wait_send()
    to_middle.wait_send()

    @pl.when(inner == 1)
    def _():
        to_outer.wait_send()
        relayed.wait_send()


def in_target_order(tile_rows, tile_cols, tile_lags, tile_scales, kept):
    ids = jnp.arange(TILES, dtype=jnp.int32)
    key = tile_rows * TILES + ids
    rank = jnp.sum((key[None, :] < key[:, None]).astype(jnp.int32), axis=1)
    at = rank[None, :] == ids[:, None]

    def placed(value):
        return jnp.sum(jnp.where(at, value[None, :], jnp.zeros_like(value)[None, :]), axis=1)

    same = (tile_rows[None, :] == tile_rows[:, None]) & (ids[None, :] < ids[:, None])
    goes_on = jnp.any(same, axis=1).astype(F32)
    info = jnp.stack([placed(ids), placed(tile_cols), placed(kept - tile_lags)])
    scales = jnp.stack([placed(tile_scales), placed(goes_on)])
    groups = jnp.arange(GROUPS, dtype=jnp.int32)
    upto = jnp.sum((tile_rows[None, :] <= groups[:, None]).astype(jnp.int32), axis=1)
    count = jnp.sum((tile_rows[None, :] == groups[:, None]).astype(jnp.int32), axis=1)
    ends = jnp.stack([jnp.maximum(upto - 1, 0), count])
    return info, scales, ends


def on_device(
    incident, past, hist_tiles, tile_rows, tile_cols, tile_lags, tile_scales, near_tiles, inverses
):
    kept = past.shape[1]
    info, scales, ends = in_target_order(
        tile_rows[0], tile_cols[0], tile_lags[0], tile_scales[0], kept
    )
    dma = pltpu.SemaphoreType.DMA
    vmem = pltpu.VMEM
    smem_spec = pl.BlockSpec(memory_space=pltpu.SMEM)
    any_spec = pl.BlockSpec(memory_space=pl.ANY)
    made = pl.pallas_call(
        kernel,
        out_shape=jax.ShapeDtypeStruct((STEPS, ILLUM, BLOCK), BF16),
        in_specs=[smem_spec] * 3 + [any_spec] * 5,
        out_specs=pl.BlockSpec(memory_space=pltpu.VMEM),
        scratch_shapes=[
            vmem((TILES, BLOCK, BLOCK), BF16),
            vmem((15, BLOCK, BLOCK), BF16),
            vmem((BLOCK, BLOCK), BF16),
            vmem((STEPS, ILLUM, BLOCK), BF16),
            vmem((8, kept, ILLUM, BLOCK), BF16),
            vmem((STEPS * ILLUM, BLOCK), F32),
            vmem((TILES, STEPS * ILLUM, BLOCK), BF16),
            vmem((STEPS, 4, 2, 4, HALF, BLOCK), BF16),
            vmem((STEPS, 4, 2, 4, HALF, BLOCK), BF16),
            vmem((2, 2, STEPS, 4, HALF, BLOCK), BF16),
            vmem((2, 2, STEPS, 2, 4, HALF, BLOCK), BF16),
            vmem((2, STEPS, 2, 4, HALF, BLOCK), BF16),
            vmem((2, 2, STEPS, HALF, BLOCK), BF16),
            vmem((2, 2, STEPS, 2, HALF, BLOCK), BF16),
            vmem((STEPS, ILLUM, BLOCK), BF16),
            vmem((STEPS, ILLUM, BLOCK), F32),
            vmem((STEPS, ILLUM, BLOCK), BF16),
            vmem((5, 6, ILLUM, BLOCK), BF16),
            vmem((3, ILLUM, BLOCK), BF16),
            vmem((STEPS, ILLUM, BLOCK), F32),
            dma((4 + TILE_PARTS,)),
            dma((4,)), dma((3,)), dma((4,)), dma((4,)),
            dma((96,)), dma((96,)), dma((4,)), dma((4,)),
            dma((4,)), dma((4,)), dma((12,)), dma((12,)),
        ],
        compiler_params=pltpu.CompilerParams(
            collective_id=0, has_side_effects=True, vmem_limit_bytes=58 * 1024 * 1024
        ),
    )(
        info, scales, ends,
        jnp.swapaxes(past[0], 1, 2),
        hist_tiles[0],
        near_tiles[0].reshape(15, BLOCK, BLOCK),
        inverses[0],
        jnp.swapaxes(incident[:, 0], 1, 2),
    )
    return jnp.swapaxes(made, 1, 2)[:, None]


def solution(mesh):
    torus = Mesh(
        mesh.devices.reshape(4, 2, 4, mesh.shape["row"], mesh.shape["cur"]), AXES
    )
    placed = (
        P(None, AXES, None, None),
        P(AXES, None, None, None),
        P(AXES, None, None, None),
        P(AXES, None),
        P(AXES, None),
        P(AXES, None),
        P(AXES, None),
        P(AXES, None, None, None, None),
        P(AXES, None, None),
    )
    return jax.shard_map(
        on_device,
        mesh=torus,
        in_specs=placed,
        out_specs=P(None, AXES, None, None),
        check_vma=False,
    )
```

```python
import functools

import jax
import jax.numpy as jnp
from jax import lax
from jax.experimental import pallas as pl
from jax.experimental.pallas import tpu as pltpu
from jax.sharding import Mesh
from jax.sharding import PartitionSpec as P

AXES = ("hist_0", "hist_1", "hist_2", "row", "cur")
MESH = pl.DeviceIdType.MESH
F32 = jnp.float32
BF16 = jnp.bfloat16
STEPS = 4
HALF = 32
ILLUM = 64
BLOCK = 256
TILES = 64
GROUPS = 32
PATCHES = 256
TILE_PARTS = 8
LAGS = 8
UNROLL = 4


def times_transposed(x, w):
    return lax.dot_general(x, w, (((1,), (1,)), ((), ())), preferred_element_type=F32)


def kernel(
    rows_ref, cols_ref, lags_ref, scales_ref,
    past_ref, tiles_ref, near_ref, inverse_ref, incident_ref,
    out_ref,
    tiles, near, inverse, incident, ga, gb, work, acc, slots, pa, pb,
    order_v, weight_v, order, weight,
    rel1, dir1, s1, rel2, dir2, ts, hist, zr, window, fresh, pre,
    local_sem, g_send, g_recv, d_send, d_recv,
    r_send, r_recv, z_send, z_recv, w_send, w_recv, n_send, n_recv,
):
    x = lax.axis_index("hist_0")
    zh = lax.axis_index("hist_1")
    y = lax.axis_index("hist_2")
    row = lax.axis_index("row")
    cur = lax.axis_index("cur")
    me = (((x * 2 + zh) * 4 + y) * 4 + row) * 2 + cur
    own = row * 2 + cur

    def patch_device(offset):
        q = lax.rem(me + offset + PATCHES, PATCHES)
        return {
            "hist_0": q // 64,
            "hist_1": lax.rem(q // 32, 2),
            "hist_2": lax.rem(q // 8, 4),
            "row": lax.rem(q // 2, 4),
            "cur": lax.rem(q, 2),
        }

    barrier = pltpu.get_barrier_semaphore()

    chunks = ((ga, 0, 6), (gb, 6, 2))
    firsts = []
    for c, (held, begin, count) in enumerate(chunks):
        firsts.append(
            pltpu.make_async_copy(
                past_ref.at[pl.ds(begin, count)], held.at[own], local_sem.at[c]
            )
        )
        firsts[c].start()
    loads = []
    part = TILES // TILE_PARTS
    for k in range(TILE_PARTS):
        loads.append(
            pltpu.make_async_copy(
                tiles_ref.at[pl.ds(k * part, part)],
                tiles.at[pl.ds(k * part, part)],
                local_sem.at[8 + k],
            )
        )
    near_load = pltpu.make_async_copy(near_ref, near, local_sem.at[4])
    inverse_load = pltpu.make_async_copy(inverse_ref, inverse, local_sem.at[5])
    incident_load = pltpu.make_async_copy(incident_ref, incident, local_sem.at[6])

    partners = [
        {"hist_0": lax.rem(x + 1, 4)},
        {"hist_0": lax.rem(x + 3, 4)},
        {"hist_2": lax.rem(y + 1, 4)},
        {"hist_2": lax.rem(y + 3, 4)},
        {"hist_1": 1 - zh},
        {"row": lax.rem(row + 1, 4)},
        {"row": lax.rem(row + 2, 4)},
        {"row": lax.rem(row + 3, 4)},
        {"cur": 1 - cur},
        patch_device(1),
        patch_device(2),
        patch_device(-1),
        patch_device(-2),
    ]
    for device in partners:
        pl.semaphore_signal(barrier, inc=1, device_id=device, device_id_type=MESH)
    pl.semaphore_wait(barrier, len(partners))
    for copy in firsts:
        copy.wait()

    def remote(src, dst, send, recv, device):
        return pltpu.make_async_remote_copy(
            src_ref=src, dst_ref=dst, send_sem=send, recv_sem=recv,
            device_id=device, device_id_type=MESH,
        )

    inner = lax.rem((row + 1) // 2, 2)
    opposite = lax.rem(row + 2, 4)
    middle = 1 + lax.rem(row, 2)
    outer = 3 * (row // 2)
    blocks = [opposite, 1 + lax.rem(row, 2), 3 - 3 * lax.rem(row, 2)]
    far = opposite * 2 + cur
    gathers = []
    for c, (held, begin, count) in enumerate(chunks):
        mine = held.at[own]
        theirs = held.at[far]
        gathers.append((
            remote(mine, mine, g_send.at[4 * c], g_recv.at[3 * c], {"row": opposite}),
            remote(mine, mine, g_send.at[4 * c + 1], g_recv.at[3 * c + 2 - inner], {"row": middle}),
            remote(mine, mine, g_send.at[4 * c + 2], g_recv.at[3 * c + 1], {"row": outer}),
            remote(theirs, theirs, g_send.at[4 * c + 3], g_recv.at[3 * c + 2], {"row": outer}),
        ))
    across = []
    for c, (held, begin, count) in enumerate(chunks):
        moved = []
        for k, block in enumerate([row] + blocks):
            spot = held.at[block * 2 + cur]
            moved.append(
                remote(spot, spot, d_send.at[4 * c + k], d_recv.at[4 * c + k], {"cur": 1 - cur})
            )
        across.append(moved)

    def send_outer(c):
        @pl.when(inner == 1)
        def _():
            gathers[c][2].start()

    gathers[0][0].start()
    gathers[0][1].start()
    send_outer(0)
    for c in range(1, 2):
        gathers[c][0].start()
        gathers[c][1].start()
    for c in range(2):
        across[c][0].start()
    for load in loads:
        load.start()
    near_load.start()
    inverse_load.start()
    incident_load.start()

    lane = lax.broadcasted_iota(jnp.int32, (TILES, TILES), 1)
    line = lax.broadcasted_iota(jnp.int32, (TILES, TILES), 0)
    nothing = jnp.zeros((TILES, TILES), jnp.int32)

    def turned(value):
        spread_out = jnp.broadcast_to(value, (TILES, TILES))
        return jnp.sum(jnp.where(lane == line, spread_out, jnp.zeros_like(spread_out)), axis=1, keepdims=True)

    targets = rows_ref[...]
    targets_down = turned(targets)
    ids = lax.broadcasted_iota(jnp.int32, (1, TILES), 1)
    begins = jnp.minimum(jnp.maximum(LAGS - lags_ref[...], 0), LAGS - STEPS)
    code = ids + TILES * (cols_ref[...] + 8 * begins)
    code_down = turned(code)
    scale_down = turned(scales_ref[...])
    key = targets * TILES + ids
    key_down = targets_down * TILES + lax.broadcasted_iota(jnp.int32, (TILES, 1), 0)
    ahead = jnp.where(jnp.broadcast_to(key, (TILES, TILES)) < key_down, nothing + 1, nothing)
    rank_down = jnp.sum(ahead, axis=1, keepdims=True)
    earlier = jnp.where((jnp.broadcast_to(targets, (TILES, TILES)) == targets_down) & (lane < line), nothing + 1, nothing)
    goes_on = jnp.sum(earlier, axis=1, keepdims=True)
    goes_on = jnp.where(goes_on > 0, jnp.ones_like(scale_down), jnp.zeros_like(scale_down))
    here = rank_down == lane
    zero = jnp.zeros((TILES, TILES), F32)
    order_v[0:1, 0:TILES] = jnp.sum(jnp.where(here, code_down, nothing), axis=0, keepdims=True)
    weight_v[0:1, 0:TILES] = jnp.sum(jnp.where(here, scale_down, zero), axis=0, keepdims=True)
    weight_v[1:2, 0:TILES] = jnp.sum(jnp.where(here, goes_on, zero), axis=0, keepdims=True)
    upto = jnp.sum(jnp.where(targets_down <= lane, nothing + 1, nothing), axis=0, keepdims=True)
    order_v[1:2, 0:TILES] = jnp.maximum(upto - 1, 0)
    order_v[2:3, 0:TILES] = jnp.sum(jnp.where(targets_down == lane, nothing + 1, nothing), axis=0, keepdims=True)
    order_copy = pltpu.make_async_copy(order_v, order, local_sem.at[7])
    weight_copy = pltpu.make_async_copy(weight_v, weight, local_sem.at[8 + TILE_PARTS])
    order_copy.start()
    weight_copy.start()
    work[...] = jnp.zeros_like(work)

    offsets = (-2, -1, 1, 2)
    window_sends = []
    for k, o in enumerate(offsets):
        for c, (src, dst) in enumerate((
            (ga.at[own, pl.ds(5, 1)], window.at[o + 2, pl.ds(0, 1)]),
            (gb.at[own], window.at[o + 2, pl.ds(1, 2)]),
        )):
            window_sends.append(
                remote(src, dst, w_send.at[2 * k + c], w_recv.at[2 * k + c], patch_device(-o))
            )

    def collect(c):
        held, begin, count = chunks[c]
        for k, block in enumerate(blocks):
            spot = held.at[block * 2 + cur]
            remote(spot, spot, g_send.at[4 * c + k], g_recv.at[3 * c + k], {"row": opposite}).wait_recv()
            if k == 0:
                @pl.when(inner == 1)
                def _():
                    gathers[c][3].start()

                if c == 0:
                    for later in range(1, 2):
                        send_outer(later)
            across[c][k + 1].start()
        for copy in across[c]:
            copy.wait_recv()
        work[:, pl.ds(begin, count)] = held[...]

    def multiply(t, count, begin_tile=0, end_tile=TILES):
        def one_tile(k, carry):
            code = order[0, k]
            tile = jnp.bitwise_and(code, TILES - 1)
            col = jnp.bitwise_and(jnp.right_shift(code, 6), 7)
            begin = jnp.right_shift(code, 9)
            held = work[col, pl.ds(begin + t, count)].reshape(count * ILLUM, BLOCK)
            term = times_transposed(held, tiles[tile]) * weight[0, k]
            total = acc[...] * weight[1, k] + term
            acc[...] = total
            slots[k, pl.ds(t, count)] = total.astype(BF16).reshape(count, ILLUM, BLOCK)
            return carry

        if begin_tile == 0:
            acc[...] = jnp.zeros_like(acc)
        lax.fori_loop(begin_tile, end_tile, one_tile, 0, unroll=UNROLL)

    def spread(t):
        def one_group(g, carry):
            value = slots[order[1, g], t]
            value = jnp.where(order[2, g] > 0, value, jnp.zeros_like(value))
            gx = g // 8
            gz = lax.rem(g // 4, 2)
            gy = lax.rem(g, 4)
            pa[t, gx, gz, gy] = value[:HALF]
            pb[t, gy, gz, gx] = value[HALF:]
            return carry

        lax.fori_loop(0, GROUPS, one_group, 0, unroll=4)

    rings = (("hist_0", x), ("hist_2", y))
    sends = []

    def ring_copy(t, stage, h, n, src, dst, device):
        index = ((t * 2 + stage) * 2 + h) * 6 + n
        copy = remote(src, dst, r_send.at[index], r_recv.at[index], device)
        sends.append(copy)
        return copy

    def ring(t, stage, h):
        axis, i = rings[(h + stage) % 2]
        right, left, over = lax.rem(i + 1, 4), lax.rem(i + 3, 4), lax.rem(i + 2, 4)
        if stage == 0:
            source = (pa, pb)[h]
            at = lambda j, z: source.at[t, j, z]
            rel, dirs = rel1, dir1
        else:
            at = lambda j, z: s1.at[h, t, z, j]
            rel, dirs = rel2, dir2
        to_right, to_left = {axis: right}, {axis: left}
        copies = (
            ring_copy(t, stage, h, 0, at(over, 0), rel.at[h, 0, t], to_right),
            ring_copy(t, stage, h, 1, at(over, 1), rel.at[h, 1, t], to_left),
            ring_copy(t, stage, h, 2, at(right, 1), dirs.at[h, 0, t, 1], to_right),
            ring_copy(t, stage, h, 3, at(left, 0), dirs.at[h, 1, t, 0], to_left),
            ring_copy(t, stage, h, 4, at(right, 0), dirs.at[h, 0, t, 0], to_right),
            ring_copy(t, stage, h, 5, at(left, 1), dirs.at[h, 1, t, 1], to_left),
        )
        return copies, at, rel, dirs, right, left, i

    state = {}

    def start(t, stage, which=(0, 1, 2, 3)):
        for h in (0, 1):
            if 0 in which:
                state[t, stage, h] = ring(t, stage, h)
        for n in which:
            for h in (0, 1):
                state[t, stage, h][0][n].start()

    def relay(t, stage):
        for n, z in ((0, 0), (1, 1)):
            for h in (0, 1):
                copies, at, rel, dirs, right, left, i = state[t, stage, h]
                copies[n].wait_recv()
                spot = at((right, left)[n], z)
                spot[...] = (spot[...].astype(F32) + rel[h, n, t].astype(F32)).astype(BF16)
                copies[4 + n].start()

    def finish_first(t):
        for h in (0, 1):
            copies, at, rel, dirs, right, left, i = state[t, 0, h]
            for n in (2, 3, 4, 5):
                copies[n].wait_recv()
            for z in (0, 1):
                total = at(i, z)[...].astype(F32) + dirs[h, 0, t, z].astype(F32)
                s1[h, t, z] = (total + dirs[h, 1, t, z].astype(F32)).astype(BF16)

    pairs = {}

    def finish_second(t):
        for h in (0, 1):
            copies, at, rel, dirs, right, left, i = state[t, 1, h]
            for n in (2, 3, 4, 5):
                copies[n].wait_recv()

        def total(h, z):
            copies, at, rel, dirs, right, left, i = state[t, 1, h]
            return at(i, z)[...].astype(F32) + dirs[h, 0, t, z].astype(F32) + dirs[h, 1, t, z].astype(F32)

        for h in (0, 1):
            ts[t, pl.ds(h * HALF, HALF)] = total(h, 1 - zh).astype(BF16)
        pairs[t] = remote(ts.at[t], zr.at[t], z_send.at[t], z_recv.at[t], {"hist_1": 1 - zh})
        sends.append(pairs[t])
        pairs[t].start()
        for h in (0, 1):
            hist[t, pl.ds(h * HALF, HALF)] = total(h, zh)

    valid = {o: jnp.logical_and(me + o >= 0, me + o < PATCHES) for o in offsets}

    def beside(o, s):
        value = window[o + 2, s + 3]
        if o == 0:
            return value
        return jnp.where(valid[o], value, jnp.zeros_like(value))

    def near_sum(lag, s, chosen):
        total = None
        for o in chosen:
            term = times_transposed(beside(o, s), near[(lag - 1) * 5 + o + 2])
            total = term if total is None else total + term
        return total

    everyone = (-2, -1, 0, 1, 2)
    rounds = {}

    def start_pre():
        near_load.wait()
        inverse_load.wait()
        incident_load.wait()
        for send in window_sends:
            send.wait_recv()
        for t in range(STEPS):
            total = incident[t].astype(F32)
            for lag in range(1, 4):
                if t - lag < 0:
                    total = total - near_sum(lag, t - lag, everyone)
            pre[t] = total

    def near_step(t):
        total = pre[t]
        if t > 0:
            for copy in rounds[t - 1]:
                copy.wait_recv()
            total = total - near_sum(1, t - 1, offsets)
        if t == 0 or True:
            pairs[t].wait_recv()
        rhs = (total - hist[t] - zr[t].astype(F32)).astype(BF16)
        made = times_transposed(rhs, inverse[...]).astype(BF16)
        out_ref[t] = made
        if t + 1 < STEPS:
            fresh[t] = made
            rounds[t] = []
            for k, o in enumerate(offsets):
                copy = remote(
                    fresh.at[t], window.at[o + 2, t + 3],
                    n_send.at[t * 4 + k], n_recv.at[t * 4 + k], patch_device(-o),
                )
                copy.start()
                rounds[t].append(copy)
                sends.append(copy)
            window[2, t + 3] = made
            pre[t + 1] = pre[t + 1] - near_sum(1, t, (0,))
        if t > 0:
            for lag in (2, 3):
                if t - 1 + lag < STEPS:
                    pre[t - 1 + lag] = pre[t - 1 + lag] - near_sum(lag, t - 1, everyone)

    collect(0)
    order_copy.wait()
    weight_copy.wait()
    for load in loads:
        load.wait()
    window[2, 0] = ga[own, 5]
    window[2, 1] = gb[own, 0]
    window[2, 2] = gb[own, 1]
    multiply(0, 2)
    spread(0)
    start(0, 0)
    spread(1)
    start(1, 0, (0, 1))
    collect(1)
    relay(0, 0)
    start(1, 0, (2, 3))
    for send in window_sends:
        send.start()
    multiply(2, 2, 0, 24)
    relay(1, 0)
    multiply(2, 2, 24, 40)
    finish_first(0)
    start(0, 1)
    multiply(2, 2, 40, 64)
    spread(2)
    start(2, 0, (0, 1))
    finish_first(1)
    start(1, 1)
    relay(0, 1)
    start(2, 0, (2, 3))
    spread(3)
    relay(2, 0)
    relay(1, 1)
    finish_second(0)
    start(3, 0, (0, 1))
    finish_second(1)
    start_pre()
    finish_first(2)
    start(2, 1)
    start(3, 0, (2, 3))
    relay(3, 0)
    relay(2, 1)
    near_step(0)
    finish_first(3)
    start(3, 1)
    finish_second(2)
    near_step(1)
    relay(3, 1)
    finish_second(3)
    near_step(2)
    near_step(3)

    for copy in sends:
        copy.wait_send()
    for copy in window_sends:
        copy.wait_send()
    for c in range(2):
        for copy in across[c]:
            copy.wait_send()
        gathers[c][0].wait_send()
        gathers[c][1].wait_send()

    @pl.when(inner == 1)
    def _():
        for c in range(2):
            gathers[c][2].wait_send()
            gathers[c][3].wait_send()


def on_device(
    incident, past, hist_tiles, tile_rows, tile_cols, tile_lags, tile_scales, near_tiles, inverses
):
    kept = past.shape[1]
    dma = pltpu.SemaphoreType.DMA
    vmem = pltpu.VMEM
    vmem_spec = pl.BlockSpec(memory_space=pltpu.VMEM)
    any_spec = pl.BlockSpec(memory_space=pl.ANY)
    made = pl.pallas_call(
        kernel,
        out_shape=jax.ShapeDtypeStruct((STEPS, ILLUM, BLOCK), BF16),
        in_specs=[vmem_spec] * 4 + [any_spec] * 5,
        out_specs=pl.BlockSpec(memory_space=pltpu.VMEM),
        scratch_shapes=[
            vmem((TILES, BLOCK, BLOCK), BF16),
            vmem((15, BLOCK, BLOCK), BF16),
            vmem((BLOCK, BLOCK), BF16),
            vmem((STEPS, ILLUM, BLOCK), BF16),
            vmem((8, 6, ILLUM, BLOCK), BF16),
            vmem((8, 2, ILLUM, BLOCK), BF16),
            vmem((8, kept, ILLUM, BLOCK), BF16),
            vmem((2 * ILLUM, BLOCK), F32),
            vmem((TILES, STEPS, ILLUM, BLOCK), BF16),
            vmem((STEPS, 4, 2, 4, HALF, BLOCK), BF16),
            vmem((STEPS, 4, 2, 4, HALF, BLOCK), BF16),
            vmem((8, 128), jnp.int32),
            vmem((8, 128), F32),
            pltpu.SMEM((8, 128), jnp.int32),
            pltpu.SMEM((8, 128), F32),
            vmem((2, 2, STEPS, 4, HALF, BLOCK), BF16),
            vmem((2, 2, STEPS, 2, 4, HALF, BLOCK), BF16),
            vmem((2, STEPS, 2, 4, HALF, BLOCK), BF16),
            vmem((2, 2, STEPS, HALF, BLOCK), BF16),
            vmem((2, 2, STEPS, 2, HALF, BLOCK), BF16),
            vmem((STEPS, ILLUM, BLOCK), BF16),
            vmem((STEPS, ILLUM, BLOCK), F32),
            vmem((STEPS, ILLUM, BLOCK), BF16),
            vmem((5, 6, ILLUM, BLOCK), BF16),
            vmem((3, ILLUM, BLOCK), BF16),
            vmem((STEPS, ILLUM, BLOCK), F32),
            dma((9 + TILE_PARTS,)),
            dma((8,)), dma((6,)), dma((8,)), dma((8,)),
            dma((96,)), dma((96,)), dma((4,)), dma((4,)),
            dma((8,)), dma((8,)), dma((12,)), dma((12,)),
        ],
        compiler_params=pltpu.CompilerParams(
            collective_id=0, has_side_effects=True, vmem_limit_bytes=58 * 1024 * 1024
        ),
    )(
        tile_rows, tile_cols, tile_lags, tile_scales,
        jnp.swapaxes(past[0], 1, 2),
        hist_tiles[0],
        near_tiles[0].reshape(15, BLOCK, BLOCK),
        inverses[0],
        jnp.swapaxes(incident[:, 0], 1, 2),
    )
    return jnp.swapaxes(made, 1, 2)[:, None]


def solution(mesh):
    torus = Mesh(
        mesh.devices.reshape(4, 2, 4, mesh.shape["row"], mesh.shape["cur"]), AXES
    )
    placed = (
        P(None, AXES, None, None),
        P(AXES, None, None, None),
        P(AXES, None, None, None),
        P(AXES, None),
        P(AXES, None),
        P(AXES, None),
        P(AXES, None),
        P(AXES, None, None, None, None),
        P(AXES, None, None),
    )
    return jax.shard_map(
        on_device,
        mesh=torus,
        in_specs=placed,
        out_specs=P(None, AXES, None, None),
        check_vma=False,
    )
```

```python
import functools

import jax
import jax.numpy as jnp
from jax import lax
from jax.experimental import pallas as pl
from jax.experimental.pallas import tpu as pltpu
from jax.sharding import Mesh
from jax.sharding import PartitionSpec as P

AXES = ("hist_0", "hist_1", "hist_2", "row", "cur")
MESH = pl.DeviceIdType.MESH
F32 = jnp.float32
BF16 = jnp.bfloat16
STEPS = 4
HALF = 32
ILLUM = 64
BLOCK = 256
TILES = 64
GROUPS = 32
PATCHES = 256
TILE_PARTS = 8
LAGS = 8
UNROLL = 8


def times_transposed(x, w):
    return lax.dot_general(x, w, (((1,), (1,)), ((), ())), preferred_element_type=F32)


def kernel(
    rows_hbm, cols_hbm, lags_hbm, scales_hbm,
    past_ref, tiles_ref, near_ref, inverse_ref, incident_ref,
    out_ref,
    tiles, near, inverse, incident, ga, gb, work, acc, slots, pa, pb,
    rows_ref, cols_ref, lags_ref, scales_ref, small_sem,
    order_v, weight_v, order, weight,
    rel1, dir1, s1, rel2, dir2, ts, hist, zr, window, fresh, pre,
    local_sem, g_send, g_recv, d_send, d_recv,
    r_send, r_recv, z_send, z_recv, w_send, w_recv, n_send, n_recv,
):
    x = lax.axis_index("hist_0")
    zh = lax.axis_index("hist_1")
    y = lax.axis_index("hist_2")
    row = lax.axis_index("row")
    cur = lax.axis_index("cur")
    me = (((x * 2 + zh) * 4 + y) * 4 + row) * 2 + cur
    own = row * 2 + cur

    def patch_device(offset):
        q = lax.rem(me + offset + PATCHES, PATCHES)
        return {
            "hist_0": q // 64,
            "hist_1": lax.rem(q // 32, 2),
            "hist_2": lax.rem(q // 8, 4),
            "row": lax.rem(q // 2, 4),
            "cur": lax.rem(q, 2),
        }

    barrier = pltpu.get_barrier_semaphore()

    chunks = ((ga, 0, 6), (gb, 6, 2))
    firsts = []
    for c, (held, begin, count) in enumerate(chunks):
        firsts.append(
            pltpu.make_async_copy(
                past_ref.at[pl.ds(begin, count)], held.at[own], local_sem.at[c]
            )
        )
        firsts[c].start()
    smalls = []
    for k, (src, dst) in enumerate((
        (rows_hbm, rows_ref), (cols_hbm, cols_ref), (lags_hbm, lags_ref), (scales_hbm, scales_ref),
    )):
        smalls.append(pltpu.make_async_copy(src, dst, small_sem.at[k]))
        smalls[k].start()
    loads = []
    part = TILES // TILE_PARTS
    for k in range(TILE_PARTS):
        loads.append(
            pltpu.make_async_copy(
                tiles_ref.at[pl.ds(k * part, part)],
                tiles.at[pl.ds(k * part, part)],
                local_sem.at[8 + k],
            )
        )
    near_load = pltpu.make_async_copy(near_ref, near, local_sem.at[4])
    inverse_load = pltpu.make_async_copy(inverse_ref, inverse, local_sem.at[5])
    incident_load = pltpu.make_async_copy(incident_ref, incident, local_sem.at[6])

    partners = [
        {"hist_0": lax.rem(x + 1, 4)},
        {"hist_0": lax.rem(x + 3, 4)},
        {"hist_2": lax.rem(y + 1, 4)},
        {"hist_2": lax.rem(y + 3, 4)},
        {"hist_1": 1 - zh},
        {"row": lax.rem(row + 1, 4)},
        {"row": lax.rem(row + 2, 4)},
        {"row": lax.rem(row + 3, 4)},
        {"cur": 1 - cur},
        patch_device(1),
        patch_device(2),
        patch_device(-1),
        patch_device(-2),
    ]
    for device in partners:
        pl.semaphore_signal(barrier, inc=1, device_id=device, device_id_type=MESH)
    pl.semaphore_wait(barrier, len(partners))
    for copy in firsts:
        copy.wait()

    def remote(src, dst, send, recv, device):
        return pltpu.make_async_remote_copy(
            src_ref=src, dst_ref=dst, send_sem=send, recv_sem=recv,
            device_id=device, device_id_type=MESH,
        )

    inner = lax.rem((row + 1) // 2, 2)
    opposite = lax.rem(row + 2, 4)
    middle = 1 + lax.rem(row, 2)
    outer = 3 * (row // 2)
    blocks = [opposite, 1 + lax.rem(row, 2), 3 - 3 * lax.rem(row, 2)]
    far = opposite * 2 + cur
    gathers = []
    for c, (held, begin, count) in enumerate(chunks):
        mine = held.at[own]
        theirs = held.at[far]
        gathers.append((
            remote(mine, mine, g_send.at[4 * c], g_recv.at[3 * c], {"row": opposite}),
            remote(mine, mine, g_send.at[4 * c + 1], g_recv.at[3 * c + 2 - inner], {"row": middle}),
            remote(mine, mine, g_send.at[4 * c + 2], g_recv.at[3 * c + 1], {"row": outer}),
            remote(theirs, theirs, g_send.at[4 * c + 3], g_recv.at[3 * c + 2], {"row": outer}),
        ))
    across = []
    for c, (held, begin, count) in enumerate(chunks):
        moved = []
        for k, block in enumerate([row] + blocks):
            spot = held.at[block * 2 + cur]
            moved.append(
                remote(spot, spot, d_send.at[4 * c + k], d_recv.at[4 * c + k], {"cur": 1 - cur})
            )
        across.append(moved)

    def send_outer(c):
        @pl.when(inner == 1)
        def _():
            gathers[c][2].start()

    gathers[0][0].start()
    gathers[0][1].start()
    send_outer(0)
    for c in range(1, 2):
        gathers[c][0].start()
        gathers[c][1].start()
    for c in range(2):
        across[c][0].start()
    for load in loads:
        load.start()
    near_load.start()
    inverse_load.start()
    incident_load.start()

    lane = lax.broadcasted_iota(jnp.int32, (TILES, TILES), 1)
    line = lax.broadcasted_iota(jnp.int32, (TILES, TILES), 0)
    nothing = jnp.zeros((TILES, TILES), jnp.int32)

    def turned(value):
        spread_out = jnp.broadcast_to(value, (TILES, TILES))
        return jnp.sum(jnp.where(lane == line, spread_out, jnp.zeros_like(spread_out)), axis=1, keepdims=True)

    for copy in smalls:
        copy.wait()
    targets = rows_ref[...]
    targets_down = turned(targets)
    ids = lax.broadcasted_iota(jnp.int32, (1, TILES), 1)
    begins = jnp.minimum(jnp.maximum(LAGS - lags_ref[...], 0), LAGS - STEPS)
    code = ids + TILES * (cols_ref[...] + 8 * begins)
    code_down = turned(code)
    scale_down = turned(scales_ref[...])
    key = targets * TILES + ids
    key_down = targets_down * TILES + lax.broadcasted_iota(jnp.int32, (TILES, 1), 0)
    ahead = jnp.where(jnp.broadcast_to(key, (TILES, TILES)) < key_down, nothing + 1, nothing)
    rank_down = jnp.sum(ahead, axis=1, keepdims=True)
    earlier = jnp.where((jnp.broadcast_to(targets, (TILES, TILES)) == targets_down) & (lane < line), nothing + 1, nothing)
    goes_on = jnp.sum(earlier, axis=1, keepdims=True)
    goes_on = jnp.where(goes_on > 0, jnp.ones_like(scale_down), jnp.zeros_like(scale_down))
    here = rank_down == lane
    zero = jnp.zeros((TILES, TILES), F32)
    order_v[0:1, 0:TILES] = jnp.sum(jnp.where(here, code_down, nothing), axis=0, keepdims=True)
    weight_v[0:1, 0:TILES] = jnp.sum(jnp.where(here, scale_down, zero), axis=0, keepdims=True)
    weight_v[1:2, 0:TILES] = jnp.sum(jnp.where(here, goes_on, zero), axis=0, keepdims=True)
    upto = jnp.sum(jnp.where(targets_down <= lane, nothing + 1, nothing), axis=0, keepdims=True)
    order_v[1:2, 0:TILES] = jnp.maximum(upto - 1, 0)
    order_v[2:3, 0:TILES] = jnp.sum(jnp.where(targets_down == lane, nothing + 1, nothing), axis=0, keepdims=True)
    order_copy = pltpu.make_async_copy(order_v, order, local_sem.at[7])
    weight_copy = pltpu.make_async_copy(weight_v, weight, local_sem.at[8 + TILE_PARTS])
    order_copy.start()
    weight_copy.start()
    work[...] = jnp.zeros_like(work)

    offsets = (-2, -1, 1, 2)
    window_sends = []
    for k, o in enumerate(offsets):
        for c, (src, dst) in enumerate((
            (ga.at[own, pl.ds(5, 1)], window.at[o + 2, pl.ds(0, 1)]),
            (gb.at[own], window.at[o + 2, pl.ds(1, 2)]),
        )):
            window_sends.append(
                remote(src, dst, w_send.at[2 * k + c], w_recv.at[2 * k + c], patch_device(-o))
            )

    def collect(c):
        held, begin, count = chunks[c]
        for k, block in enumerate(blocks):
            spot = held.at[block * 2 + cur]
            remote(spot, spot, g_send.at[4 * c + k], g_recv.at[3 * c + k], {"row": opposite}).wait_recv()
            if k == 0:
                @pl.when(inner == 1)
                def _():
                    gathers[c][3].start()

                if c == 0:
                    for later in range(1, 2):
                        send_outer(later)
            across[c][k + 1].start()
        for copy in across[c]:
            copy.wait_recv()
        work[:, pl.ds(begin, count)] = held[...]

    def multiply(t, count, begin_tile=0, end_tile=TILES):
        def one_tile(k, carry):
            code = order[0, k]
            tile = jnp.bitwise_and(code, TILES - 1)
            col = jnp.bitwise_and(jnp.right_shift(code, 6), 7)
            begin = jnp.right_shift(code, 9)
            held = work[col, pl.ds(begin + t, count)].reshape(count * ILLUM, BLOCK)
            term = times_transposed(held, tiles[tile]) * weight[0, k]
            total = acc[...] * weight[1, k] + term
            acc[...] = total
            slots[k, pl.ds(t, count)] = total.astype(BF16).reshape(count, ILLUM, BLOCK)
            return carry

        if begin_tile == 0:
            acc[...] = jnp.zeros_like(acc)
        lax.fori_loop(begin_tile, end_tile, one_tile, 0, unroll=UNROLL)

    def spread(t):
        def one_group(g, carry):
            value = slots[order[1, g], t]
            value = jnp.where(order[2, g] > 0, value, jnp.zeros_like(value))
            gx = g // 8
            gz = lax.rem(g // 4, 2)
            gy = lax.rem(g, 4)
            pa[t, gx, gz, gy] = value[:HALF]
            pb[t, gy, gz, gx] = value[HALF:]
            return carry

        lax.fori_loop(0, GROUPS, one_group, 0, unroll=4)

    rings = (("hist_0", x), ("hist_2", y))
    sends = []

    def ring_copy(t, stage, h, n, src, dst, device):
        index = ((t * 2 + stage) * 2 + h) * 6 + n
        copy = remote(src, dst, r_send.at[index], r_recv.at[index], device)
        sends.append(copy)
        return copy

    def ring(t, stage, h):
        axis, i = rings[(h + stage) % 2]
        right, left, over = lax.rem(i + 1, 4), lax.rem(i + 3, 4), lax.rem(i + 2, 4)
        if stage == 0:
            source = (pa, pb)[h]
            at = lambda j, z: source.at[t, j, z]
            rel, dirs = rel1, dir1
        else:
            at = lambda j, z: s1.at[h, t, z, j]
            rel, dirs = rel2, dir2
        to_right, to_left = {axis: right}, {axis: left}
        copies = (
            ring_copy(t, stage, h, 0, at(over, 0), rel.at[h, 0, t], to_right),
            ring_copy(t, stage, h, 1, at(over, 1), rel.at[h, 1, t], to_left),
            ring_copy(t, stage, h, 2, at(right, 1), dirs.at[h, 0, t, 1], to_right),
            ring_copy(t, stage, h, 3, at(left, 0), dirs.at[h, 1, t, 0], to_left),
            ring_copy(t, stage, h, 4, at(right, 0), dirs.at[h, 0, t, 0], to_right),
            ring_copy(t, stage, h, 5, at(left, 1), dirs.at[h, 1, t, 1], to_left),
        )
        return copies, at, rel, dirs, right, left, i

    state = {}

    def start(t, stage, which=(0, 1, 2, 3)):
        for h in (0, 1):
            if 0 in which:
                state[t, stage, h] = ring(t, stage, h)
        for n in which:
            for h in (0, 1):
                state[t, stage, h][0][n].start()

    def relay(t, stage):
        for n, z in ((0, 0), (1, 1)):
            for h in (0, 1):
                copies, at, rel, dirs, right, left, i = state[t, stage, h]
                copies[n].wait_recv()
                spot = at((right, left)[n], z)
                spot[...] = (spot[...].astype(F32) + rel[h, n, t].astype(F32)).astype(BF16)
                copies[4 + n].start()

    def finish_first(t):
        for h in (0, 1):
            copies, at, rel, dirs, right, left, i = state[t, 0, h]
            for n in (2, 3, 4, 5):
                copies[n].wait_recv()
            for z in (0, 1):
                total = at(i, z)[...].astype(F32) + dirs[h, 0, t, z].astype(F32)
                s1[h, t, z] = (total + dirs[h, 1, t, z].astype(F32)).astype(BF16)

    pairs = {}

    def finish_second(t):
        for h in (0, 1):
            copies, at, rel, dirs, right, left, i = state[t, 1, h]
            for n in (2, 3, 4, 5):
                copies[n].wait_recv()

        def total(h, z):
            copies, at, rel, dirs, right, left, i = state[t, 1, h]
            return at(i, z)[...].astype(F32) + dirs[h, 0, t, z].astype(F32) + dirs[h, 1, t, z].astype(F32)

        for h in (0, 1):
            ts[t, pl.ds(h * HALF, HALF)] = total(h, 1 - zh).astype(BF16)
        pairs[t] = remote(ts.at[t], zr.at[t], z_send.at[t], z_recv.at[t], {"hist_1": 1 - zh})
        sends.append(pairs[t])
        pairs[t].start()
        for h in (0, 1):
            hist[t, pl.ds(h * HALF, HALF)] = total(h, zh)

    valid = {o: jnp.logical_and(me + o >= 0, me + o < PATCHES) for o in offsets}

    def beside(o, s):
        value = window[o + 2, s + 3]
        if o == 0:
            return value
        return jnp.where(valid[o], value, jnp.zeros_like(value))

    def near_sum(lag, s, chosen):
        total = None
        for o in chosen:
            term = times_transposed(beside(o, s), near[(lag - 1) * 5 + o + 2])
            total = term if total is None else total + term
        return total

    everyone = (-2, -1, 0, 1, 2)
    rounds = {}

    def start_pre():
        near_load.wait()
        inverse_load.wait()
        incident_load.wait()
        for send in window_sends:
            send.wait_recv()
        for t in range(STEPS):
            total = incident[t].astype(F32)
            for lag in range(1, 4):
                if t - lag < 0:
                    total = total - near_sum(lag, t - lag, everyone)
            pre[t] = total

    def near_step(t):
        total = pre[t]
        if t > 0:
            for copy in rounds[t - 1]:
                copy.wait_recv()
            total = total - near_sum(1, t - 1, offsets)
        if t == 0 or True:
            pairs[t].wait_recv()
        rhs = (total - hist[t] - zr[t].astype(F32)).astype(BF16)
        made = times_transposed(rhs, inverse[...]).astype(BF16)
        out_ref[t] = made
        if t + 1 < STEPS:
            fresh[t] = made
            rounds[t] = []
            for k, o in enumerate(offsets):
                copy = remote(
                    fresh.at[t], window.at[o + 2, t + 3],
                    n_send.at[t * 4 + k], n_recv.at[t * 4 + k], patch_device(-o),
                )
                copy.start()
                rounds[t].append(copy)
                sends.append(copy)
            window[2, t + 3] = made
            pre[t + 1] = pre[t + 1] - near_sum(1, t, (0,))
        if t > 0:
            for lag in (2, 3):
                if t - 1 + lag < STEPS:
                    pre[t - 1 + lag] = pre[t - 1 + lag] - near_sum(lag, t - 1, everyone)

    collect(0)
    order_copy.wait()
    weight_copy.wait()
    for load in loads:
        load.wait()
    window[2, 0] = ga[own, 5]
    window[2, 1] = gb[own, 0]
    window[2, 2] = gb[own, 1]
    for send in window_sends:
        send.start()
    multiply(0, 2)
    spread(0)
    start(0, 0)
    spread(1)
    start(1, 0, (0, 1))
    collect(1)
    relay(0, 0)
    start(1, 0, (2, 3))
    multiply(2, 2, 0, 40)
    relay(1, 0)
    multiply(2, 2, 40, 48)
    finish_first(0)
    start(0, 1)
    multiply(2, 2, 48, 64)
    spread(2)
    start(2, 0, (0, 1))
    finish_first(1)
    start(1, 1)
    relay(0, 1)
    start(2, 0, (2, 3))
    spread(3)
    start_pre()
    relay(2, 0)
    finish_second(0)
    relay(1, 1)
    start(3, 0)
    finish_first(2)
    start(2, 1)
    finish_second(1)
    near_step(0)
    relay(3, 0)
    relay(2, 1)
    finish_second(2)
    near_step(1)
    finish_first(3)
    start(3, 1)
    relay(3, 1)
    near_step(2)
    finish_second(3)
    near_step(3)

    for copy in sends:
        copy.wait_send()
    for copy in window_sends:
        copy.wait_send()
    for c in range(2):
        for copy in across[c]:
            copy.wait_send()
        gathers[c][0].wait_send()
        gathers[c][1].wait_send()

    @pl.when(inner == 1)
    def _():
        for c in range(2):
            gathers[c][2].wait_send()
            gathers[c][3].wait_send()


def on_device(
    incident, past, hist_tiles, tile_rows, tile_cols, tile_lags, tile_scales, near_tiles, inverses
):
    kept = past.shape[1]
    dma = pltpu.SemaphoreType.DMA
    vmem = pltpu.VMEM
    any_spec = pl.BlockSpec(memory_space=pl.ANY)
    made = pl.pallas_call(
        kernel,
        out_shape=jax.ShapeDtypeStruct((STEPS, ILLUM, BLOCK), BF16),
        in_specs=[any_spec] * 9,
        out_specs=pl.BlockSpec(memory_space=pltpu.VMEM),
        scratch_shapes=[
            vmem((TILES, BLOCK, BLOCK), BF16),
            vmem((15, BLOCK, BLOCK), BF16),
            vmem((BLOCK, BLOCK), BF16),
            vmem((STEPS, ILLUM, BLOCK), BF16),
            vmem((8, 6, ILLUM, BLOCK), BF16),
            vmem((8, 2, ILLUM, BLOCK), BF16),
            vmem((8, kept, ILLUM, BLOCK), BF16),
            vmem((2 * ILLUM, BLOCK), F32),
            vmem((TILES, STEPS, ILLUM, BLOCK), BF16),
            vmem((STEPS, 4, 2, 4, HALF, BLOCK), BF16),
            vmem((STEPS, 4, 2, 4, HALF, BLOCK), BF16),
            vmem((1, TILES), jnp.int32),
            vmem((1, TILES), jnp.int32),
            vmem((1, TILES), jnp.int32),
            vmem((1, TILES), F32),
            dma((4,)),
            vmem((8, 128), jnp.int32),
            vmem((8, 128), F32),
            pltpu.SMEM((8, 128), jnp.int32),
            pltpu.SMEM((8, 128), F32),
            vmem((2, 2, STEPS, 4, HALF, BLOCK), BF16),
            vmem((2, 2, STEPS, 2, 4, HALF, BLOCK), BF16),
            vmem((2, STEPS, 2, 4, HALF, BLOCK), BF16),
            vmem((2, 2, STEPS, HALF, BLOCK), BF16),
            vmem((2, 2, STEPS, 2, HALF, BLOCK), BF16),
            vmem((STEPS, ILLUM, BLOCK), BF16),
            vmem((STEPS, ILLUM, BLOCK), F32),
            vmem((STEPS, ILLUM, BLOCK), BF16),
            vmem((5, 6, ILLUM, BLOCK), BF16),
            vmem((3, ILLUM, BLOCK), BF16),
            vmem((STEPS, ILLUM, BLOCK), F32),
            dma((9 + TILE_PARTS,)),
            dma((8,)), dma((6,)), dma((8,)), dma((8,)),
            dma((96,)), dma((96,)), dma((4,)), dma((4,)),
            dma((8,)), dma((8,)), dma((12,)), dma((12,)),
        ],
        compiler_params=pltpu.CompilerParams(
            collective_id=0, has_side_effects=True, vmem_limit_bytes=58 * 1024 * 1024
        ),
    )(
        tile_rows, tile_cols, tile_lags, tile_scales,
        jnp.swapaxes(past[0], 1, 2),
        hist_tiles[0],
        near_tiles[0].reshape(15, BLOCK, BLOCK),
        inverses[0],
        jnp.swapaxes(incident[:, 0], 1, 2),
    )
    return jnp.swapaxes(made, 1, 2)[:, None]


def solution(mesh):
    torus = Mesh(
        mesh.devices.reshape(4, 2, 4, mesh.shape["row"], mesh.shape["cur"]), AXES
    )
    placed = (
        P(None, AXES, None, None),
        P(AXES, None, None, None),
        P(AXES, None, None, None),
        P(AXES, None),
        P(AXES, None),
        P(AXES, None),
        P(AXES, None),
        P(AXES, None, None, None, None),
        P(AXES, None, None),
    )
    return jax.shard_map(
        on_device,
        mesh=torus,
        in_specs=placed,
        out_specs=P(None, AXES, None, None),
        check_vma=False,
    )
```

```python
import functools

import jax
import jax.numpy as jnp
from jax import lax
from jax.experimental import pallas as pl
from jax.experimental.pallas import tpu as pltpu
from jax.sharding import Mesh
from jax.sharding import PartitionSpec as P

AXES = ("hist_0", "hist_1", "hist_2", "row", "cur")
MESH = pl.DeviceIdType.MESH
F32 = jnp.float32
BF16 = jnp.bfloat16
STEPS = 4
HALF = 32
ILLUM = 64
BLOCK = 256
TILES = 64
GROUPS = 32
PATCHES = 256
TILE_PARTS = 8
LAGS = 8
UNROLL = 8


def times_transposed(x, w):
    return lax.dot_general(x, w, (((1,), (1,)), ((), ())), preferred_element_type=F32)


def kernel(
    rows_hbm, cols_hbm, lags_hbm, scales_hbm,
    past_ref, tiles_ref, near_ref, inverse_ref, incident_ref,
    out_ref,
    tiles, near, inverse, incident, ga, gb, work, acc, slots, pa, pb,
    rows_ref, cols_ref, lags_ref, scales_ref, small_sem,
    order_v, weight_v, order, weight,
    rel1, dir1, s1, rel2, dir2, ts, hist, zr, window, fresh, pre,
    local_sem, g_send, g_recv, d_send, d_recv,
    r_send, r_recv, z_send, z_recv, w_send, w_recv, n_send, n_recv,
):
    x = lax.axis_index("hist_0")
    zh = lax.axis_index("hist_1")
    y = lax.axis_index("hist_2")
    row = lax.axis_index("row")
    cur = lax.axis_index("cur")
    me = (((x * 2 + zh) * 4 + y) * 4 + row) * 2 + cur
    own = row * 2 + cur

    def patch_device(offset):
        q = lax.rem(me + offset + PATCHES, PATCHES)
        return {
            "hist_0": q // 64,
            "hist_1": lax.rem(q // 32, 2),
            "hist_2": lax.rem(q // 8, 4),
            "row": lax.rem(q // 2, 4),
            "cur": lax.rem(q, 2),
        }

    barrier = pltpu.get_barrier_semaphore()

    chunks = ((ga, 0, 6), (gb, 6, 2))
    firsts = []
    for c, (held, begin, count) in enumerate(chunks):
        firsts.append(
            pltpu.make_async_copy(
                past_ref.at[pl.ds(begin, count)], held.at[own], local_sem.at[c]
            )
        )
        firsts[c].start()
    smalls = []
    for k, (src, dst) in enumerate((
        (rows_hbm, rows_ref), (cols_hbm, cols_ref), (lags_hbm, lags_ref), (scales_hbm, scales_ref),
    )):
        smalls.append(pltpu.make_async_copy(src, dst, small_sem.at[k]))
        smalls[k].start()
    loads = []
    part = TILES // TILE_PARTS
    for k in range(TILE_PARTS):
        loads.append(
            pltpu.make_async_copy(
                tiles_ref.at[pl.ds(k * part, part)],
                tiles.at[pl.ds(k * part, part)],
                local_sem.at[8 + k],
            )
        )
    near_load = pltpu.make_async_copy(near_ref, near, local_sem.at[4])
    inverse_load = pltpu.make_async_copy(inverse_ref, inverse, local_sem.at[5])
    incident_load = pltpu.make_async_copy(incident_ref, incident, local_sem.at[6])

    partners = [
        {"hist_0": lax.rem(x + 1, 4)},
        {"hist_0": lax.rem(x + 3, 4)},
        {"hist_2": lax.rem(y + 1, 4)},
        {"hist_2": lax.rem(y + 3, 4)},
        {"hist_1": 1 - zh},
        {"row": lax.rem(row + 1, 4)},
        {"row": lax.rem(row + 2, 4)},
        {"row": lax.rem(row + 3, 4)},
        {"cur": 1 - cur},
        patch_device(1),
        patch_device(2),
        patch_device(-1),
        patch_device(-2),
    ]
    for device in partners:
        pl.semaphore_signal(barrier, inc=1, device_id=device, device_id_type=MESH)
    pl.semaphore_wait(barrier, len(partners))
    for copy in firsts:
        copy.wait()

    def remote(src, dst, send, recv, device):
        return pltpu.make_async_remote_copy(
            src_ref=src, dst_ref=dst, send_sem=send, recv_sem=recv,
            device_id=device, device_id_type=MESH,
        )

    inner = lax.rem((row + 1) // 2, 2)
    opposite = lax.rem(row + 2, 4)
    middle = 1 + lax.rem(row, 2)
    outer = 3 * (row // 2)
    blocks = [opposite, 1 + lax.rem(row, 2), 3 - 3 * lax.rem(row, 2)]
    far = opposite * 2 + cur
    gathers = []
    for c, (held, begin, count) in enumerate(chunks):
        mine = held.at[own]
        theirs = held.at[far]
        gathers.append((
            remote(mine, mine, g_send.at[4 * c], g_recv.at[3 * c], {"row": opposite}),
            remote(mine, mine, g_send.at[4 * c + 1], g_recv.at[3 * c + 2 - inner], {"row": middle}),
            remote(mine, mine, g_send.at[4 * c + 2], g_recv.at[3 * c + 1], {"row": outer}),
            remote(theirs, theirs, g_send.at[4 * c + 3], g_recv.at[3 * c + 2], {"row": outer}),
        ))
    across = []
    for c, (held, begin, count) in enumerate(chunks):
        moved = []
        for k, block in enumerate([row] + blocks):
            spot = held.at[block * 2 + cur]
            moved.append(
                remote(spot, spot, d_send.at[4 * c + k], d_recv.at[4 * c + k], {"cur": 1 - cur})
            )
        across.append(moved)

    def send_outer(c):
        @pl.when(inner == 1)
        def _():
            gathers[c][2].start()

    gathers[0][0].start()
    gathers[0][1].start()
    send_outer(0)
    for c in range(1, 2):
        gathers[c][0].start()
        gathers[c][1].start()
    for c in range(2):
        across[c][0].start()
    for load in loads:
        load.start()
    near_load.start()
    inverse_load.start()
    incident_load.start()

    lane = lax.broadcasted_iota(jnp.int32, (TILES, TILES), 1)
    line = lax.broadcasted_iota(jnp.int32, (TILES, TILES), 0)
    nothing = jnp.zeros((TILES, TILES), jnp.int32)

    def turned(value):
        spread_out = jnp.broadcast_to(value, (TILES, TILES))
        return jnp.sum(jnp.where(lane == line, spread_out, jnp.zeros_like(spread_out)), axis=1, keepdims=True)

    for copy in smalls:
        copy.wait()
    targets = rows_ref[...]
    targets_down = turned(targets)
    ids = lax.broadcasted_iota(jnp.int32, (1, TILES), 1)
    begins = jnp.minimum(jnp.maximum(LAGS - lags_ref[...], 0), LAGS - STEPS)
    code = ids + TILES * (cols_ref[...] + 8 * begins)
    code_down = turned(code)
    scale_down = turned(scales_ref[...])
    key = targets * TILES + ids
    key_down = targets_down * TILES + lax.broadcasted_iota(jnp.int32, (TILES, 1), 0)
    ahead = jnp.where(jnp.broadcast_to(key, (TILES, TILES)) < key_down, nothing + 1, nothing)
    rank_down = jnp.sum(ahead, axis=1, keepdims=True)
    earlier = jnp.where((jnp.broadcast_to(targets, (TILES, TILES)) == targets_down) & (lane < line), nothing + 1, nothing)
    goes_on = jnp.sum(earlier, axis=1, keepdims=True)
    goes_on = jnp.where(goes_on > 0, jnp.ones_like(scale_down), jnp.zeros_like(scale_down))
    here = rank_down == lane
    zero = jnp.zeros((TILES, TILES), F32)
    order_v[0:1, 0:TILES] = jnp.sum(jnp.where(here, code_down, nothing), axis=0, keepdims=True)
    weight_v[0:1, 0:TILES] = jnp.sum(jnp.where(here, scale_down, zero), axis=0, keepdims=True)
    weight_v[1:2, 0:TILES] = jnp.sum(jnp.where(here, goes_on, zero), axis=0, keepdims=True)
    upto = jnp.sum(jnp.where(targets_down <= lane, nothing + 1, nothing), axis=0, keepdims=True)
    order_v[1:2, 0:TILES] = jnp.maximum(upto - 1, 0)
    order_v[2:3, 0:TILES] = jnp.sum(jnp.where(targets_down == lane, nothing + 1, nothing), axis=0, keepdims=True)
    order_copy = pltpu.make_async_copy(order_v, order, local_sem.at[7])
    weight_copy = pltpu.make_async_copy(weight_v, weight, local_sem.at[8 + TILE_PARTS])
    order_copy.start()
    weight_copy.start()
    work[...] = jnp.zeros_like(work)

    offsets = (-2, -1, 1, 2)
    window_sends = []
    for k, o in enumerate(offsets):
        for c, (src, dst) in enumerate((
            (ga.at[own, pl.ds(5, 1)], window.at[o + 2, pl.ds(0, 1)]),
            (gb.at[own], window.at[o + 2, pl.ds(1, 2)]),
        )):
            window_sends.append(
                remote(src, dst, w_send.at[2 * k + c], w_recv.at[2 * k + c], patch_device(-o))
            )

    def collect(c):
        held, begin, count = chunks[c]
        for k, block in enumerate(blocks):
            spot = held.at[block * 2 + cur]
            remote(spot, spot, g_send.at[4 * c + k], g_recv.at[3 * c + k], {"row": opposite}).wait_recv()
            if k == 0:
                @pl.when(inner == 1)
                def _():
                    gathers[c][3].start()

                if c == 0:
                    for later in range(1, 2):
                        send_outer(later)
            across[c][k + 1].start()
        for copy in across[c]:
            copy.wait_recv()
        work[:, pl.ds(begin, count)] = held[...]

    def multiply(t, count, begin_tile=0, end_tile=TILES):
        def one_tile(k, carry):
            code = order[0, k]
            tile = jnp.bitwise_and(code, TILES - 1)
            col = jnp.bitwise_and(jnp.right_shift(code, 6), 7)
            begin = jnp.right_shift(code, 9)
            held = work[col, pl.ds(begin + t, count)].reshape(count * ILLUM, BLOCK)
            term = times_transposed(held, tiles[tile]) * weight[0, k]
            total = acc[...] * weight[1, k] + term
            acc[...] = total
            slots[k, pl.ds(t, count)] = total.astype(BF16).reshape(count, ILLUM, BLOCK)
            return carry

        if begin_tile == 0:
            acc[...] = jnp.zeros_like(acc)
        lax.fori_loop(begin_tile, end_tile, one_tile, 0, unroll=UNROLL)

    def spread(t):
        def one_group(g, carry):
            value = slots[order[1, g], t]
            value = jnp.where(order[2, g] > 0, value, jnp.zeros_like(value))
            gx = g // 8
            gz = lax.rem(g // 4, 2)
            gy = lax.rem(g, 4)
            pa[t, gx, gz, gy] = value[:HALF]
            pb[t, gy, gz, gx] = value[HALF:]
            return carry

        lax.fori_loop(0, GROUPS, one_group, 0, unroll=4)

    rings = (("hist_0", x), ("hist_2", y))
    sends = []

    def ring_copy(t, stage, h, n, src, dst, device):
        index = ((t * 2 + stage) * 2 + h) * 6 + n
        copy = remote(src, dst, r_send.at[index], r_recv.at[index], device)
        sends.append(copy)
        return copy

    def ring(t, stage, h):
        axis, i = rings[(h + stage) % 2]
        right, left, over = lax.rem(i + 1, 4), lax.rem(i + 3, 4), lax.rem(i + 2, 4)
        if stage == 0:
            source = (pa, pb)[h]
            at = lambda j, z: source.at[t, j, z]
            rel, dirs = rel1, dir1
        else:
            at = lambda j, z: s1.at[h, t, z, j]
            rel, dirs = rel2, dir2
        to_right, to_left = {axis: right}, {axis: left}
        copies = (
            ring_copy(t, stage, h, 0, at(over, 0), rel.at[h, 0, t], to_right),
            ring_copy(t, stage, h, 1, at(over, 1), rel.at[h, 1, t], to_left),
            ring_copy(t, stage, h, 2, at(right, 1), dirs.at[h, 0, t, 1], to_right),
            ring_copy(t, stage, h, 3, at(left, 0), dirs.at[h, 1, t, 0], to_left),
            ring_copy(t, stage, h, 4, at(right, 0), dirs.at[h, 0, t, 0], to_right),
            ring_copy(t, stage, h, 5, at(left, 1), dirs.at[h, 1, t, 1], to_left),
        )
        return copies, at, rel, dirs, right, left, i

    state = {}

    def start(t, stage, which=(0, 1, 2, 3)):
        for h in (0, 1):
            if 0 in which:
                state[t, stage, h] = ring(t, stage, h)
        for n in which:
            for h in (0, 1):
                state[t, stage, h][0][n].start()

    def relay(t, stage):
        for n, z in ((0, 0), (1, 1)):
            for h in (0, 1):
                copies, at, rel, dirs, right, left, i = state[t, stage, h]
                copies[n].wait_recv()
                spot = at((right, left)[n], z)
                spot[...] = (spot[...].astype(F32) + rel[h, n, t].astype(F32)).astype(BF16)
                copies[4 + n].start()

    def finish_first(t):
        for h in (0, 1):
            copies, at, rel, dirs, right, left, i = state[t, 0, h]
            for n in (2, 3, 4, 5):
                copies[n].wait_recv()
            for z in (0, 1):
                total = at(i, z)[...].astype(F32) + dirs[h, 0, t, z].astype(F32)
                s1[h, t, z] = (total + dirs[h, 1, t, z].astype(F32)).astype(BF16)

    pairs = {}

    def finish_second(t):
        for h in (0, 1):
            copies, at, rel, dirs, right, left, i = state[t, 1, h]
            for n in (2, 3, 4, 5):
                copies[n].wait_recv()

        def total(h, z):
            copies, at, rel, dirs, right, left, i = state[t, 1, h]
            return at(i, z)[...].astype(F32) + dirs[h, 0, t, z].astype(F32) + dirs[h, 1, t, z].astype(F32)

        for h in (0, 1):
            ts[t, pl.ds(h * HALF, HALF)] = total(h, 1 - zh).astype(BF16)
        pairs[t] = remote(ts.at[t], zr.at[t], z_send.at[t], z_recv.at[t], {"hist_1": 1 - zh})
        sends.append(pairs[t])
        pairs[t].start()
        for h in (0, 1):
            hist[t, pl.ds(h * HALF, HALF)] = total(h, zh)

    valid = {o: jnp.logical_and(me + o >= 0, me + o < PATCHES) for o in offsets}

    def beside(o, s):
        value = window[o + 2, s + 3]
        if o == 0:
            return value
        return jnp.where(valid[o], value, jnp.zeros_like(value))

    def near_sum(lag, s, chosen):
        total = None
        for o in chosen:
            term = times_transposed(beside(o, s), near[(lag - 1) * 5 + o + 2])
            total = term if total is None else total + term
        return total

    everyone = (-2, -1, 0, 1, 2)
    rounds = {}

    def start_pre():
        near_load.wait()
        inverse_load.wait()
        incident_load.wait()
        for send in window_sends:
            send.wait_recv()
        known_before(0)

    def known_before(t):
        total = incident[t].astype(F32)
        for lag in range(1, 4):
            if t - lag < 0:
                total = total - near_sum(lag, t - lag, everyone)
        pre[t] = total

    def near_step(t):
        pairs[t].wait_recv()
        total = pre[t] - hist[t] - zr[t].astype(F32)
        if t > 0:
            for k in (1, 2, 0, 3):
                rounds[t - 1][k].wait_recv()
                total = total - near_sum(1, t - 1, (offsets[k],))
        rhs = total.astype(BF16)
        made = times_transposed(rhs, inverse[...]).astype(BF16)
        out_ref[t] = made
        if t + 1 < STEPS:
            fresh[t] = made
            rounds[t] = []
            for k, o in enumerate(offsets):
                copy = remote(
                    fresh.at[t], window.at[o + 2, t + 3],
                    n_send.at[t * 4 + k], n_recv.at[t * 4 + k], patch_device(-o),
                )
                copy.start()
                rounds[t].append(copy)
                sends.append(copy)
            window[2, t + 3] = made
            if t == 0:
                for later in range(1, STEPS):
                    known_before(later)
            pre[t + 1] = pre[t + 1] - near_sum(1, t, (0,))
        if t > 0:
            for lag in (2, 3):
                if t - 1 + lag < STEPS:
                    pre[t - 1 + lag] = pre[t - 1 + lag] - near_sum(lag, t - 1, everyone)

    collect(0)
    order_copy.wait()
    weight_copy.wait()
    for load in loads:
        load.wait()
    window[2, 0] = ga[own, 5]
    window[2, 1] = gb[own, 0]
    window[2, 2] = gb[own, 1]
    for send in window_sends:
        send.start()
    multiply(0, 2)
    spread(0)
    start(0, 0)
    spread(1)
    start(1, 0, (0, 1))
    collect(1)
    relay(0, 0)
    start(1, 0, (2, 3))
    multiply(2, 2, 0, 40)
    relay(1, 0)
    multiply(2, 2, 40, 48)
    finish_first(0)
    start(0, 1)
    multiply(2, 2, 48, 64)
    spread(2)
    start(2, 0, (0, 1))
    finish_first(1)
    start(1, 1)
    relay(0, 1)
    start(2, 0, (2, 3))
    spread(3)
    start_pre()
    relay(2, 0)
    finish_second(0)
    relay(1, 1)
    start(3, 0)
    finish_first(2)
    start(2, 1)
    finish_second(1)
    near_step(0)
    relay(3, 0)
    relay(2, 1)
    finish_second(2)
    near_step(1)
    finish_first(3)
    start(3, 1)
    relay(3, 1)
    near_step(2)
    finish_second(3)
    near_step(3)

    for copy in sends:
        copy.wait_send()
    for copy in window_sends:
        copy.wait_send()
    for c in range(2):
        for copy in across[c]:
            copy.wait_send()
        gathers[c][0].wait_send()
        gathers[c][1].wait_send()

    @pl.when(inner == 1)
    def _():
        for c in range(2):
            gathers[c][2].wait_send()
            gathers[c][3].wait_send()


def on_device(
    incident, past, hist_tiles, tile_rows, tile_cols, tile_lags, tile_scales, near_tiles, inverses
):
    kept = past.shape[1]
    dma = pltpu.SemaphoreType.DMA
    vmem = pltpu.VMEM
    any_spec = pl.BlockSpec(memory_space=pl.ANY)
    made = pl.pallas_call(
        kernel,
        out_shape=jax.ShapeDtypeStruct((STEPS, ILLUM, BLOCK), BF16),
        in_specs=[any_spec] * 9,
        out_specs=pl.BlockSpec(memory_space=pltpu.VMEM),
        scratch_shapes=[
            vmem((TILES, BLOCK, BLOCK), BF16),
            vmem((15, BLOCK, BLOCK), BF16),
            vmem((BLOCK, BLOCK), BF16),
            vmem((STEPS, ILLUM, BLOCK), BF16),
            vmem((8, 6, ILLUM, BLOCK), BF16),
            vmem((8, 2, ILLUM, BLOCK), BF16),
            vmem((8, kept, ILLUM, BLOCK), BF16),
            vmem((2 * ILLUM, BLOCK), F32),
            vmem((TILES, STEPS, ILLUM, BLOCK), BF16),
            vmem((STEPS, 4, 2, 4, HALF, BLOCK), BF16),
            vmem((STEPS, 4, 2, 4, HALF, BLOCK), BF16),
            vmem((1, TILES), jnp.int32),
            vmem((1, TILES), jnp.int32),
            vmem((1, TILES), jnp.int32),
            vmem((1, TILES), F32),
            dma((4,)),
            vmem((8, 128), jnp.int32),
            vmem((8, 128), F32),
            pltpu.SMEM((8, 128), jnp.int32),
            pltpu.SMEM((8, 128), F32),
            vmem((2, 2, STEPS, 4, HALF, BLOCK), BF16),
            vmem((2, 2, STEPS, 2, 4, HALF, BLOCK), BF16),
            vmem((2, STEPS, 2, 4, HALF, BLOCK), BF16),
            vmem((2, 2, STEPS, HALF, BLOCK), BF16),
            vmem((2, 2, STEPS, 2, HALF, BLOCK), BF16),
            vmem((STEPS, ILLUM, BLOCK), BF16),
            vmem((STEPS, ILLUM, BLOCK), F32),
            vmem((STEPS, ILLUM, BLOCK), BF16),
            vmem((5, 6, ILLUM, BLOCK), BF16),
            vmem((3, ILLUM, BLOCK), BF16),
            vmem((STEPS, ILLUM, BLOCK), F32),
            dma((9 + TILE_PARTS,)),
            dma((8,)), dma((6,)), dma((8,)), dma((8,)),
            dma((96,)), dma((96,)), dma((4,)), dma((4,)),
            dma((8,)), dma((8,)), dma((12,)), dma((12,)),
        ],
        compiler_params=pltpu.CompilerParams(
            collective_id=0, has_side_effects=True, vmem_limit_bytes=58 * 1024 * 1024
        ),
    )(
        tile_rows, tile_cols, tile_lags, tile_scales,
        jnp.swapaxes(past[0], 1, 2),
        hist_tiles[0],
        near_tiles[0].reshape(15, BLOCK, BLOCK),
        inverses[0],
        jnp.swapaxes(incident[:, 0], 1, 2),
    )
    return jnp.swapaxes(made, 1, 2)[:, None]


def solution(mesh):
    torus = Mesh(
        mesh.devices.reshape(4, 2, 4, mesh.shape["row"], mesh.shape["cur"]), AXES
    )
    placed = (
        P(None, AXES, None, None),
        P(AXES, None, None, None),
        P(AXES, None, None, None),
        P(AXES, None),
        P(AXES, None),
        P(AXES, None),
        P(AXES, None),
        P(AXES, None, None, None, None),
        P(AXES, None, None),
    )
    return jax.shard_map(
        on_device,
        mesh=torus,
        in_specs=placed,
        out_specs=P(None, AXES, None, None),
        check_vma=False,
    )
```
